128 devices in a mesh: tp: 4 (over x), dp: 32 (over z, y, core).
Axes of the slice: x: 4, y: 4, z: 4, core: 2. Of those that a mesh axis runs over, the one named last changes fastest.
Arguments:
- hidden: bfloat16 [32, 512, 1280], P('dp')
- ln_gamma: float32 [1280], replicated
- ln_beta: float32 [1280], replicated
- embed_table: bfloat16 [50304, 1280], P('tp')
- labels: int32 [32, 512], P('dp')
- loss_mask: int32 [32, 512], P('dp')
Outputs:
- output 1: float32 [], replicated
- output 2: bfloat16 [32, 512, 1280], P('dp')
- output 3: float32 [50304, 1280], P('tp')
- output 4: float32 [1280], replicated
- output 5: float32 [1280], replicated
All inputs are finite; a program needn't handle non-finite values.
Results may differ from the reference program's by a relative error of at most 0.001.
Values sent between devices are 32-bit elements.
A program may use at most 1 GiB of HBM per device.

```python
import jax
import jax.numpy as jnp
from jax import lax

HIDDEN = 1280
VOCAB_SIZE = 50304
NUM_SEQS = 32
SEQ_LEN = 512
TOKEN_BLOCK = min(SEQ_LEN, 128)
LAYER_EPS = 1e-5
SCORE_SCALE = 3.5


def setup_inputs(seed: int = 0) -> dict:
    rand_keys = jax.random.split(jax.random.key(seed), 6)
    hidden = (1.5 * jax.random.normal(rand_keys[0], (NUM_SEQS, SEQ_LEN, HIDDEN), jnp.float32)).astype(jnp.bfloat16)
    ln_gamma = 1.0 + 0.3 * jax.random.normal(rand_keys[1], (HIDDEN,), jnp.float32)
    ln_beta = 0.3 * jax.random.normal(rand_keys[2], (HIDDEN,), jnp.float32)
    embed_table = (SCORE_SCALE * HIDDEN ** -0.5 * jax.random.normal(rand_keys[3], (VOCAB_SIZE, HIDDEN), jnp.float32)).astype(jnp.bfloat16)
    labels = jax.random.randint(rand_keys[4], (NUM_SEQS, SEQ_LEN), 0, VOCAB_SIZE, jnp.int32)
    lengths = jax.random.randint(rand_keys[5], (NUM_SEQS, 1), 1, SEQ_LEN + 1, jnp.int32)
    positions = jnp.arange(SEQ_LEN, dtype=jnp.int32)[None, :]
    loss_mask = (positions < lengths).astype(jnp.int32)
    return {'hidden': hidden, 'ln_gamma': ln_gamma, 'ln_beta': ln_beta, 'embed_table': embed_table, 'labels': labels, 'loss_mask': loss_mask}


def reference(hidden, ln_gamma, ln_beta, embed_table, labels, loss_mask):
    mask_float = loss_mask.astype(jnp.float32)
    token_count = jnp.sum(mask_float)
    vocab_ids = jnp.arange(VOCAB_SIZE, dtype=jnp.int32)[None, :]
    block_hidden = hidden.reshape(-1, TOKEN_BLOCK, HIDDEN)
    block_labels = labels.reshape(-1, TOKEN_BLOCK)
    block_mask = mask_float.reshape(-1, TOKEN_BLOCK, 1)

    def block_step(scan_carry, block_data):
        d_embed, d_gamma, d_beta, loss_sum = scan_carry
        block_rows, row_labels, row_mask = block_data
        x_float = block_rows.astype(jnp.float32)
        row_mean = jnp.mean(x_float, axis=-1, keepdims=True)
        centered = x_float - row_mean
        inv_std = lax.rsqrt(jnp.mean(centered * centered, axis=-1, keepdims=True) + LAYER_EPS)
        x_hat = centered * inv_std
        normed = (x_hat * ln_gamma + ln_beta).astype(jnp.bfloat16)
        logits = jnp.dot(normed, embed_table.T, preferred_element_type=jnp.float32)
        row_max = jnp.max(logits, axis=-1, keepdims=True)
        log_norm = row_max + jnp.log(jnp.sum(jnp.exp(logits - row_max), axis=-1, keepdims=True))
        is_target = vocab_ids == row_labels[:, None]
        target_logit = jnp.sum(jnp.where(is_target, logits, 0.0), axis=-1, keepdims=True)
        loss_sum = loss_sum + jnp.sum(row_mask * (log_norm - target_logit))
        soft_probs = jnp.exp(logits - log_norm)
        grad_logits = (jnp.where(is_target, soft_probs - 1.0, soft_probs) * (row_mask / token_count)).astype(jnp.bfloat16)
        grad_normed = jnp.dot(grad_logits, embed_table, preferred_element_type=jnp.float32)
        d_embed = d_embed + jnp.dot(grad_logits.T, normed, preferred_element_type=jnp.float32)
        d_gamma = d_gamma + jnp.sum(grad_normed * x_hat, axis=0)
        d_beta = d_beta + jnp.sum(grad_normed, axis=0)
        grad_scaled = grad_normed * ln_gamma
        grad_x = (grad_scaled - jnp.mean(grad_scaled, axis=-1, keepdims=True) - x_hat * jnp.mean(grad_scaled * x_hat, axis=-1, keepdims=True)) * inv_std
        return (d_embed, d_gamma, d_beta, loss_sum), grad_x.astype(jnp.bfloat16)

    zero_carry = (jnp.zeros((VOCAB_SIZE, HIDDEN), jnp.float32), jnp.zeros((HIDDEN,), jnp.float32), jnp.zeros((HIDDEN,), jnp.float32), jnp.zeros((), jnp.float32))
    final_carry, grad_blocks = lax.scan(block_step, zero_carry, (block_hidden, block_labels, block_mask))
    d_embed, d_gamma, d_beta, loss_sum = final_carry
    d_hidden = grad_blocks.reshape(NUM_SEQS, SEQ_LEN, HIDDEN)
    return loss_sum / token_count, d_hidden, d_embed, d_gamma, d_beta
```

```python
import functools

import jax
import jax.numpy as jnp
from jax import lax
from jax.experimental import pallas as pl
from jax.experimental.pallas import tpu as pltpu
from jax.sharding import Mesh, PartitionSpec as P

LAYER_EPS = 1e-5
SHARD = 12576
HALF = 6400
GROUP = 1600
BLOCK = 400
CUT = 176
TOK = 512
DIM = 1280
AXES = ('tp', 'z', 'y', 'c')
VMEM_LIMIT = 60 * 1024 * 1024


def index_of(x, z, y, c):
    return ((x % 4 * 4 + z % 4) * 4 + y % 4) * 2 + c % 2


def make_perm(move):
    pairs = []
    for x in range(4):
        for z in range(4):
            for y in range(4):
                for c in range(2):
                    pairs.append((index_of(x, z, y, c), index_of(*move(x, z, y, c))))
    return pairs


def on_ring(axis, step):
    def move(x, z, y, c):
        along_y = (axis == 'A') == (c == 0)
        return (x, z, y + step, c) if along_y else (x, z + step, y, c)
    return make_perm(move)


SIB = make_perm(lambda x, z, y, c: (x, z, y, 1 - c))
RING = {(axis, step): on_ring(axis, step) for axis in 'AB' for step in (1, -1, 2)}
for _s in (1, -1, 2):
    RING['X', _s] = make_perm(lambda x, z, y, c, s=_s: (x + s, z, y, c))


def send(value, pairs):
    return lax.ppermute(value, AXES, pairs)


def dot_nt(a, b):
    return lax.dot_general(a, b, (((1,), (1,)), ((), ())), preferred_element_type=jnp.float32)


def stats_kernel(at_ref, own_ref, sib_ref, e_ref, out_ref, z_ref, e_buf, sems, *, tile, steps):
    start, low = at_ref[0], at_ref[1]

    def fetch(i, slot):
        rows = pl.ds(pl.multiple_of(start + i * tile, 32), tile)
        return pltpu.make_async_copy(e_ref.at[rows], e_buf.at[slot], sems.at[slot])

    fetch(0, 0).start()
    z_ref[:TOK] = own_ref[...].astype(jnp.bfloat16)
    z_ref[TOK:] = sib_ref[...].astype(jnp.bfloat16)

    def update(i, slot, carry, masked):
        top, total = carry
        logits = dot_nt(e_buf[slot], z_ref[...])
        if masked:
            rows = lax.broadcasted_iota(jnp.int32, logits.shape, 0)
            logits = jnp.where(rows >= low, logits, -jnp.inf)
        logits = logits.reshape(tile // 8, 8, 2 * TOK)
        new_top = jnp.maximum(top, jnp.max(logits, axis=0))
        total = total * jnp.exp(top - new_top) + jnp.sum(jnp.exp(logits - new_top[None]), axis=0)
        return new_top, total

    fetch(1, 1).start()
    fetch(0, 0).wait()
    carry = (jnp.full((8, 2 * TOK), -jnp.inf, jnp.float32), jnp.zeros((8, 2 * TOK), jnp.float32))
    carry = update(0, 0, carry, True)

    def body(i, carry):
        slot = lax.rem(i, 2)

        @pl.when(i + 1 < steps)
        def _():
            fetch(i + 1, 1 - slot).start()
        fetch(i, slot).wait()
        return update(i, slot, carry, False)

    top, total = lax.fori_loop(1, steps, body, carry)
    all_top = jnp.max(top, axis=0, keepdims=True)
    all_total = jnp.sum(total * jnp.exp(top - all_top), axis=0, keepdims=True)
    out_ref[...] = jnp.zeros_like(out_ref)
    out_ref[0:1] = all_top
    out_ref[1:2] = all_total


def logit_stats(start, low, own, sib, embed):
    tile, steps = 640, HALF // 640
    return pl.pallas_call(
        functools.partial(stats_kernel, tile=tile, steps=steps),
        name='logit_stats',
        out_shape=jax.ShapeDtypeStruct((8, 2 * TOK), jnp.float32),
        in_specs=[
            pl.BlockSpec(memory_space=pltpu.SMEM),
            pl.BlockSpec(memory_space=pltpu.VMEM),
            pl.BlockSpec(memory_space=pltpu.VMEM),
            pl.BlockSpec(memory_space=pl.ANY),
        ],
        out_specs=pl.BlockSpec(memory_space=pltpu.VMEM),
        scratch_shapes=[
            pltpu.VMEM((2 * TOK, DIM), jnp.bfloat16),
            pltpu.VMEM((2, tile, DIM), jnp.bfloat16),
            pltpu.SemaphoreType.DMA((2,)),
        ],
        compiler_params=pltpu.CompilerParams(vmem_limit_bytes=VMEM_LIMIT),
        cost_estimate=pl.CostEstimate(flops=2 * 1024 * HALF * DIM, bytes_accessed=HALF * DIM * 2, transcendentals=HALF * 1024),
    )(jnp.stack([start, low]).astype(jnp.int32), own, sib, embed)


PIECES = ((0, 400), (400, 200), (600, 200), (800, 200), (1000, 200), (1200, 200), (1400, 200))


def vgrad_kernel(*refs, pieces, first, last):
    refs = list(refs)
    at_ref = refs.pop(0)
    z_in = [refs.pop(0) for _ in range(pieces)]
    info_ref, e_ref = refs.pop(0), refs.pop(0)
    acc_in = None if first else refs.pop(0)
    outs = [refs.pop(0) for _ in range(len(PIECES) if last else 1)]
    z_raw, z_ref, e_buf, acc, z_sems, e_sems, acc_sems, out_sems = refs
    tokens = pieces * TOK

    z_copies = [pltpu.make_async_copy(z_in[p], z_raw.at[p], z_sems.at[p]) for p in range(pieces)]
    e_copies = []
    for j in range(4):
        head = pl.multiple_of(at_ref[2 * j], 16)
        tail = pl.multiple_of(at_ref[2 * j + 1], 16)
        e_copies.append((
            pltpu.make_async_copy(e_ref.at[pl.ds(head, CUT)], e_buf.at[j, pl.ds(0, CUT)], e_sems.at[j, 0]),
            pltpu.make_async_copy(e_ref.at[pl.ds(tail, BLOCK - CUT)], e_buf.at[j, pl.ds(CUT, BLOCK - CUT)], e_sems.at[j, 1]),
        ))
    z_copies[0].start()
    for copy in e_copies[0]:
        copy.start()
    for copy in z_copies[1:]:
        copy.start()
    acc_copies = []
    for j in range(4):
        if j:
            for copy in e_copies[j]:
                copy.start()
        if acc_in is not None:
            rows = pl.ds(j * BLOCK, BLOCK)
            acc_copies.append(pltpu.make_async_copy(acc_in.at[rows], acc.at[rows], acc_sems.at[j]))
            acc_copies[-1].start()
    for p in range(pieces):
        z_copies[p].wait()
        z_ref[p * TOK:(p + 1) * TOK] = z_raw[p].astype(jnp.bfloat16)

    lse = info_ref[0:1]
    scale = info_ref[1:2]
    labels = info_ref[2:3].astype(jnp.int32)
    out_copies = []
    for j in range(4):
        for copy in e_copies[j]:
            copy.wait()
        logits = dot_nt(e_buf[j], z_ref[...])
        local = lax.broadcasted_iota(jnp.int32, (BLOCK, tokens), 0) + at_ref[8 + j]
        probs = jnp.exp(logits - lse)
        grad = (jnp.where(local == labels, probs - 1.0, probs) * scale).astype(jnp.bfloat16)
        part = jnp.dot(grad, z_ref[...], preferred_element_type=jnp.float32)
        rows = slice(j * BLOCK, (j + 1) * BLOCK)
        if acc_in is None:
            acc[rows] = part
        else:
            acc_copies[j].wait()
            acc[rows] += part
        if last:
            for k, (at, size) in enumerate(PIECES):
                if at // BLOCK == j:
                    out_copies.append(pltpu.make_async_copy(acc.at[pl.ds(at, size)], outs[k], out_sems.at[k]))
                    out_copies[-1].start()
        else:
            span = pl.ds(j * BLOCK, BLOCK)
            out_copies.append(pltpu.make_async_copy(acc.at[span], outs[0].at[span], out_sems.at[j]))
            out_copies[-1].start()
    for copy in out_copies:
        copy.wait()


def vocab_grad(at, z_list, info, embed, acc, last):
    pieces = len(z_list)
    first = acc is None
    tokens = pieces * TOK
    if last:
        out_shape = [jax.ShapeDtypeStruct((size, DIM), jnp.float32) for _, size in PIECES]
    else:
        out_shape = [jax.ShapeDtypeStruct((GROUP, DIM), jnp.float32)]
    any_spec = pl.BlockSpec(memory_space=pl.ANY)
    return pl.pallas_call(
        functools.partial(vgrad_kernel, pieces=pieces, first=first, last=last),
        name=f'vocab_grad_{pieces}_{int(first)}{int(last)}',
        out_shape=out_shape,
        in_specs=[pl.BlockSpec(memory_space=pltpu.SMEM)] + [any_spec] * pieces
        + [pl.BlockSpec(memory_space=pltpu.VMEM), any_spec] + [any_spec] * (0 if first else 1),
        out_specs=[any_spec] * len(out_shape),
        scratch_shapes=[
            pltpu.VMEM((pieces, TOK, DIM), jnp.float32),
            pltpu.VMEM((tokens, DIM), jnp.bfloat16),
            pltpu.VMEM((4, BLOCK, DIM), jnp.bfloat16),
            pltpu.VMEM((GROUP, DIM), jnp.float32),
            pltpu.SemaphoreType.DMA((pieces,)),
            pltpu.SemaphoreType.DMA((4, 2)),
            pltpu.SemaphoreType.DMA((4,)),
            pltpu.SemaphoreType.DMA((len(PIECES),)),
        ],
        compiler_params=pltpu.CompilerParams(vmem_limit_bytes=VMEM_LIMIT),
        cost_estimate=pl.CostEstimate(flops=4 * tokens * GROUP * DIM, bytes_accessed=GROUP * DIM * 10, transcendentals=GROUP * tokens),
    )(at, *z_list, info, embed, *([] if first else [acc]))


def dz_kernel(at_ref, own_ref, sib_ref, lse_ref, scale_ref, label_ref, mask_ref, e_ref, own_out, sib_out, hit_ref,
              z_ref, e_buf, logit_buf, grad_buf, acc, sems, *, tile, steps):
    start, low = at_ref[0], at_ref[1]

    def fetch(i, slot):
        rows = pl.ds(pl.multiple_of(start + i * tile, 32), tile)
        return pltpu.make_async_copy(e_ref.at[rows], e_buf.at[slot], sems.at[slot])

    fetch(0, 0).start()
    z_ref[:TOK] = own_ref[...].astype(jnp.bfloat16)
    z_ref[TOK:] = sib_ref[...].astype(jnp.bfloat16)
    acc[...] = jnp.zeros_like(acc)
    hit_ref[...] = jnp.zeros_like(hit_ref)

    def body(i, carry):
        slot = lax.rem(i, 2)

        @pl.when(i + 1 < steps)
        def _():
            fetch(i + 1, 1 - slot).start()
        fetch(i, slot).wait()
        logit_buf[...] = dot_nt(z_ref[...], e_buf[slot])
        for k in range(tile // 128):
            lanes = slice(k * 128, (k + 1) * 128)
            logits = logit_buf[:, lanes]
            row = lax.broadcasted_iota(jnp.int32, logits.shape, 1) + (i * tile + k * 128)
            probs = jnp.exp(logits - lse_ref[...])
            target = row + start == label_ref[...]
            valid = row >= low
            grad = jnp.where(target, probs - 1.0, probs) * scale_ref[...]
            grad_buf[:, lanes] = jnp.where(valid, grad, 0.0).astype(jnp.bfloat16)
            hit = jnp.where(target & valid, logits * mask_ref[...], 0.0)
            hit_ref[...] += jnp.sum(hit.reshape(2 * TOK // 8, 8, 128), axis=0)
        acc[...] += jnp.dot(grad_buf[...], e_buf[slot], preferred_element_type=jnp.float32)
        return carry

    lax.fori_loop(0, steps, body, 0)
    own_out[...] = acc[:TOK]
    sib_out[...] = acc[TOK:]


def token_grad(start, low, own, sib, cols, embed):
    tile, steps = 1280, HALF // 1280
    vmem = pl.BlockSpec(memory_space=pltpu.VMEM)
    return pl.pallas_call(
        functools.partial(dz_kernel, tile=tile, steps=steps),
        name='token_grad',
        out_shape=[
            jax.ShapeDtypeStruct((TOK, DIM), jnp.float32),
            jax.ShapeDtypeStruct((TOK, DIM), jnp.float32),
            jax.ShapeDtypeStruct((8, 128), jnp.float32),
        ],
        in_specs=[pl.BlockSpec(memory_space=pltpu.SMEM)] + [vmem] * 6 + [pl.BlockSpec(memory_space=pl.ANY)],
        out_specs=[vmem] * 3,
        scratch_shapes=[
            pltpu.VMEM((2 * TOK, DIM), jnp.bfloat16),
            pltpu.VMEM((2, tile, DIM), jnp.bfloat16),
            pltpu.VMEM((2 * TOK, tile), jnp.float32),
            pltpu.VMEM((2 * TOK, tile), jnp.bfloat16),
            pltpu.VMEM((2 * TOK, DIM), jnp.float32),
            pltpu.SemaphoreType.DMA((2,)),
        ],
        compiler_params=pltpu.CompilerParams(vmem_limit_bytes=VMEM_LIMIT),
        cost_estimate=pl.CostEstimate(flops=4 * 1024 * HALF * DIM, bytes_accessed=HALF * DIM * 2, transcendentals=HALF * 1024),
    )(jnp.stack([start, low]).astype(jnp.int32), own, sib, *cols, embed)


def place_kernel(*refs, blocks, first):
    if first:
        at_ref, src_ref, out_ref, buf, in_sems, out_sems = refs
    else:
        at_ref, src_ref, _, out_ref, buf, in_sems, out_sems = refs
    parts = ((0, CUT), (CUT, BLOCK - CUT))
    for j in range(blocks):
        for k, (at, size) in enumerate(parts):
            rows = pl.ds(j * BLOCK + at, size)
            pltpu.make_async_copy(src_ref.at[rows], buf.at[rows], in_sems.at[j, k]).start()
    for j in range(blocks):
        for k, (at, size) in enumerate(parts):
            rows = pl.ds(j * BLOCK + at, size)
            pltpu.make_async_copy(src_ref.at[rows], buf.at[rows], in_sems.at[j, k]).wait()
            to = pl.ds(pl.multiple_of(at_ref[2 * j] + at, 16), size)

            @pl.when((at_ref[2 * j + 1] == 1) | (k == 0))
            def _():
                pltpu.make_async_copy(buf.at[rows], out_ref.at[to], out_sems.at[j, k]).start()
    for j in range(blocks):
        for k, (at, size) in enumerate(parts):
            rows = pl.ds(j * BLOCK + at, size)
            to = pl.ds(pl.multiple_of(at_ref[2 * j] + at, 16), size)

            @pl.when((at_ref[2 * j + 1] == 1) | (k == 0))
            def _():
                pltpu.make_async_copy(buf.at[rows], out_ref.at[to], out_sems.at[j, k]).wait()


def place(at, src, out):
    blocks = src.shape[0] // BLOCK
    any_spec = pl.BlockSpec(memory_space=pl.ANY)
    first = out is None
    return pl.pallas_call(
        functools.partial(place_kernel, blocks=blocks, first=first),
        name=f'place_{blocks}_{int(first)}',
        out_shape=jax.ShapeDtypeStruct((SHARD, DIM), jnp.float32),
        in_specs=[pl.BlockSpec(memory_space=pltpu.SMEM), any_spec] + [any_spec] * (0 if first else 1),
        out_specs=any_spec,
        input_output_aliases={} if first else {2: 0},
        scratch_shapes=[
            pltpu.VMEM((blocks * BLOCK, DIM), jnp.float32),
            pltpu.SemaphoreType.DMA((blocks, 2)),
            pltpu.SemaphoreType.DMA((blocks, 2)),
        ],
        compiler_params=pltpu.CompilerParams(vmem_limit_bytes=VMEM_LIMIT),
        cost_estimate=pl.CostEstimate(flops=blocks * 5_000_000_000 // 4, bytes_accessed=blocks * BLOCK * DIM * 8, transcendentals=0),
    )(at, src, *([] if first else [out]))


def block_rows(c, a, b):
    a, b = a % 4, b % 4
    row = HALF * c + GROUP * a + BLOCK * b
    full = 1 - ((c == 1) & (a == 3) & (b == 3)).astype(jnp.int32)
    return row, full


def place_at(c, a, b, count):
    values = []
    for j in range(count):
        values.extend(block_rows(c, a, b + j))
    return jnp.stack(values).astype(jnp.int32)


def sum_over_dp(value):
    value = value + send(value, SIB)
    for axis in ('y', 'z'):
        parts = [lax.ppermute(value, axis, [(i, (i + s) % 4) for i in range(4)]) for s in (1, 2, 3)]
        me = lax.axis_index(axis)
        terms = jnp.stack([value] + parts)
        order = jnp.stack([terms[(me - i) % 4] for i in range(4)])
        value = (order[0] + order[1]) + (order[2] + order[3])
    return value


def solution(mesh):
    mesh4 = Mesh(mesh.devices.reshape(4, 4, 4, 2), AXES)

    def local_step(hidden, ln_gamma, ln_beta, embed, labels, loss_mask):
        hidden, labels, mask = hidden[0], labels[0], loss_mask[0].astype(jnp.float32)
        x, z, y, c = (lax.axis_index(n) for n in AXES)
        a = jnp.where(c == 0, y, z)
        b = jnp.where(c == 0, z, y)

        token_count = sum_over_dp(jnp.broadcast_to(jnp.sum(mask), (8, 128)))[0, 0]

        x_float = hidden.astype(jnp.float32)
        row_mean = jnp.mean(x_float, axis=-1, keepdims=True)
        centered = x_float - row_mean
        inv_std = lax.rsqrt(jnp.mean(centered * centered, axis=-1, keepdims=True) + LAYER_EPS)
        x_hat = centered * inv_std
        own = (x_hat * ln_gamma + ln_beta).astype(jnp.bfloat16).astype(jnp.float32)

        sib = send(own, SIB)
        left_own, right_own = send(own, RING['A', 1]), send(own, RING['A', -1])
        left_sib, right_sib = send(sib, RING['A', 1]), send(sib, RING['A', -1])
        opp_own, opp_sib = send(left_own, RING['A', 1]), send(right_sib, RING['A', -1])

        start, low = c * (SHARD - HALF), c * (2 * HALF - SHARD)
        stats = logit_stats(start, low, own, sib, embed)
        theirs = send(stats, SIB)
        theirs = jnp.concatenate([theirs[:, TOK:], theirs[:, :TOK]], axis=1)

        def merge(p, q):
            top = jnp.maximum(p[0:1], q[0:1])
            total = p[1:2] * jnp.exp(p[0:1] - top) + q[1:2] * jnp.exp(q[0:1] - top)
            return jnp.concatenate([top, total, jnp.zeros((6, 2 * TOK), jnp.float32)], axis=0)

        first = jnp.where(c == 0, stats, theirs)
        second = jnp.where(c == 0, theirs, stats)
        chip = merge(first, second)
        parts = jnp.stack([chip] + [send(chip, RING['X', s]) for s in (1, 2, -1)])
        order = [parts[(x - i) % 4] for i in range(4)]
        whole = merge(merge(order[0], order[1]), merge(order[2], order[3]))
        lse = whole[0] + jnp.log(whole[1])

        tags = jnp.concatenate([mask[None], labels[None].astype(jnp.float32), jnp.zeros((6, TOK), jnp.float32)], axis=0)
        tags = jnp.concatenate([tags, send(tags, SIB)], axis=1)
        mask2, label2 = tags[0], tags[1]
        scale = mask2 / token_count
        info = jnp.concatenate([lse[None], scale[None], label2[None], jnp.zeros((5, 2 * TOK), jnp.float32)], axis=0)
        left_info, right_info, opp_info = (send(info, RING['A', s]) for s in (1, -1, 2))

        base = x * SHARD
        ats, firsts = [], []
        for j in range(4):
            row, _ = block_rows(c, a, b + j)
            ats.extend([row, jnp.minimum(row + CUT, SHARD - (BLOCK - CUT))])
            firsts.append(base + row)
        at = jnp.stack(ats + firsts).astype(jnp.int32)
        acc, = vocab_grad(at, [own, sib], info, embed, None, False)
        acc, = vocab_grad(at, [left_own, left_sib, right_own, right_sib],
                          jnp.concatenate([left_info, right_info], axis=1), embed, acc, False)
        mine, right_lo, right_hi, opp_lo, opp_hi, left_lo, left_hi = vocab_grad(
            at, [opp_own, opp_sib], opp_info, embed, acc, True)

        from_left = send(opp_lo, RING['B', 1])
        from_right = send(opp_hi, RING['B', -1])
        plain_hi = send(right_hi, RING['B', 1])
        plain_lo = send(left_lo, RING['B', -1])
        sum_lo = send(right_lo + from_left, RING['B', 1])
        sum_hi = send(left_hi + from_right, RING['B', -1])
        block_lo = mine[:200] + (sum_lo + plain_lo)
        block_hi = mine[200:] + (plain_hi + sum_hi)

        left_lo, left_hi = send(block_lo, RING['B', 1]), send(block_hi, RING['B', 1])
        right_lo, right_hi = send(block_lo, RING['B', -1]), send(block_hi, RING['B', -1])
        opp_lo = send(left_lo, RING['B', 1])
        opp_hi = send(right_hi, RING['B', -1])
        group = jnp.concatenate([block_lo, block_hi, right_lo, right_hi, opp_lo, opp_hi, left_lo, left_hi], axis=0)

        left, right = send(group, RING['A', 1]), send(group, RING['A', -1])
        opp_1 = send(left[:800], RING['A', 1])
        opp_2 = send(right[800:], RING['A', -1])

        tied, group_tie = lax.optimization_barrier((own, block_lo))
        spread = lambda v: jnp.broadcast_to(v[:, None], (2 * TOK, 128))
        cols = [spread(lse), spread(scale), spread(label2.astype(jnp.int32) - base), spread(mask2)]
        dz_own, dz_sib, hits = token_grad(start, low, tied, sib, cols, embed)
        dz = dz_own + send(dz_sib, SIB)
        quarters = dz.reshape(4, TOK // 4, DIM)
        quarter = lambda s: lax.dynamic_index_in_dim(quarters, (x + s) % 4, 0, keepdims=False)
        mine_q = quarter(0) + send(quarter(1), RING['X', 1]) + send(quarter(3), RING['X', -1]) + send(quarter(2), RING['X', 2])
        got = [mine_q, send(mine_q, RING['X', -1]), send(mine_q, RING['X', 2]), send(mine_q, RING['X', 1])]
        got = jnp.stack(got)
        grad_normed = jnp.concatenate([lax.dynamic_index_in_dim(got, (q - x) % 4, 0, keepdims=False) for q in range(4)], axis=0)
        grad_scaled = grad_normed * ln_gamma
        d_hidden = (grad_scaled - jnp.mean(grad_scaled, axis=-1, keepdims=True)
                    - x_hat * jnp.mean(grad_scaled * x_hat, axis=-1, keepdims=True)) * inv_std
        d_gamma = jnp.sum(grad_normed * x_hat, axis=0)
        d_beta = jnp.sum(grad_normed, axis=0)

        hit = jnp.broadcast_to(jnp.sum(hits), (8, 128))
        hit = hit + sum(send(hit, RING['X', s]) for s in (1, 2, -1))
        lse_sum = jnp.sum(mask * lse[:TOK])
        tail = jnp.concatenate([
            jnp.broadcast_to(lse_sum, (128,)), hit[0],
            d_gamma, d_beta, jnp.zeros((4 * 128,), jnp.float32)]).reshape(26, 128)
        tail = sum_over_dp(tail).reshape(-1)
        loss_sum = tail[0] - tail[128]
        d_gamma, d_beta = tail[256:256 + DIM], tail[256 + DIM:256 + 2 * DIM]

        out = place(place_at(c, a, b, 4), group, None)
        out = place(place_at(1 - c, b, a, 4), send(group, SIB), out)
        out = place(place_at(c, a - 1, b, 4), left, out)
        out = place(place_at(c, a + 1, b, 4), right, out)
        out = place(place_at(1 - c, b - 1, a, 4), send(left, SIB), out)
        out = place(place_at(1 - c, b + 1, a, 4), send(right, SIB), out)
        out = place(place_at(c, a + 2, b, 2), opp_1, out)
        out = place(place_at(c, a + 2, b + 2, 2), opp_2, out)
        out = place(place_at(1 - c, b + 2, a, 2), send(opp_1, SIB), out)
        out = place(place_at(1 - c, b + 2, a + 2, 2), send(opp_2, SIB), out)
        return loss_sum / token_count, d_hidden.astype(jnp.bfloat16)[None], out, d_gamma, d_beta

    dp = ('z', 'y', 'c')
    return jax.shard_map(
        local_step, mesh=mesh4,
        in_specs=(P(dp, None, None), P(None), P(None), P('tp', None), P(dp, None), P(dp, None)),
        out_specs=(P(), P(dp, None, None), P('tp', None), P(None), P(None)),
        check_vma=False)
```

```python
import functools
import itertools

import jax
import jax.numpy as jnp
import numpy as np
from jax import lax
from jax.experimental import pallas as pl
from jax.experimental.pallas import tpu as pltpu
from jax.sharding import Mesh, PartitionSpec as P

LAYER_EPS = 1e-5
SHARD = 12576
HALF = 6400
GROUP = 1600
BLOCK = 400
CUT = 176
TOK = 512
DIM = 1280
AXES = ('tp', 'z', 'y', 'c')
VMEM_LIMIT = 60 * 1024 * 1024
T2_EARLY, T2_LATE = 6, 7
KERNEL_VMEM = 63 * 1024 * 1024
PLACE_FLOPS = 1_500_000_000


SIZES = (4, 4, 4, 2)


def make_perm(move):
    return [(i, int(np.ravel_multi_index(move(*at), SIZES, mode='wrap'))) for i, at in enumerate(np.ndindex(SIZES))]


def on_ring(axis, step):
    def move(x, z, y, c):
        along_y = (axis == 'A') == (c == 0)
        return (x, z, y + step, c) if along_y else (x, z + step, y, c)
    return make_perm(move)


SIB = make_perm(lambda x, z, y, c: (x, z, y, 1 - c))
RING_RIGHT, RING_LEFT = on_ring('A', 1), on_ring('A', -1)


def send(value, pairs):
    return lax.ppermute(value, AXES, pairs)


def dot_nt(a, b):
    return lax.dot_general(a, b, (((1,), (1,)), ((), ())), preferred_element_type=jnp.float32)


E_TILE = 1280
T1_SUB = 320
HALF_BLOCK = BLOCK // 2
QUARTER = TOK // 4
OVERLAP = 2 * HALF - SHARD
MESH_ID = pl.DeviceIdType.MESH
STEPS = (1, 3, 2)
OWN, RIGHT, OPPOSITE, LEFT = range(4)
SEMS = 200


def in_order(ref):
    return (ref[0] + ref[1]) + (ref[2] + ref[3])


def merge(p, q):
    top = jnp.maximum(p[0], q[0])
    return top, p[1] * jnp.exp(p[0] - top) + q[1] * jnp.exp(q[0] - top)


def top_total(ref):
    return ref[0:1], ref[1:2]


def head_kernel(*refs, t2_early, t2_late):
    refs = iter(refs)
    take = lambda n: [next(refs) for _ in range(n)]
    hid_ref, gamma_ref, beta_ref, tags_ref, e_ref = take(5)
    dh_out, tail_out, land = take(3)
    groups = [take(4) for _ in range(3)]
    others = [take(4) for _ in range(3)]
    (zf, zf_sib, stage, zb, e_grp, e_tile, acc, dz_acc, dz_in, x_parts, g_buf, cols,
     tag, inf, st_c, st_x, counts, rs_in, rs_out, hits, x_hits, t_core, t_ring, t_swap,
     e_sem, stage_sem, sems) = refs
    free = itertools.count()
    x, z, y, c = (lax.axis_index(n) for n in AXES)
    b = (1 - c) * z + c * y
    a = (1 - c) * y + c * z
    sib = (x, z, y, 1 - c)
    ring_a = {s: (x, lax.rem(z + c * s, 4), lax.rem(y + (1 - c) * s, 4), c) for s in STEPS}
    ring_b = {s: (x, lax.rem(z + (1 - c) * s, 4), lax.rem(y + c * s, 4), c) for s in STEPS}
    ring_x = {s: (lax.rem(x + s, 4), z, y, c) for s in STEPS}
    right, left, opposite = STEPS
    start, low = c * (SHARD - HALF), c * OVERLAP
    base = x * SHARD

    def remote(src, dst, device):
        return pltpu.make_async_remote_copy(
            src_ref=src, dst_ref=dst, send_sem=sems.at[next(free)], recv_sem=sems.at[next(free)],
            device_id=device, device_id_type=MESH_ID)

    def local(src, dst):
        return pltpu.make_async_copy(src, dst, sems.at[next(free)])

    def to_ring(src, dst, ring):
        return [remote(src, dst, ring[s]) for s in STEPS]

    def start_all(copies):
        for copy in copies:
            copy.start()

    def wait_all(copies):
        for copy in copies:
            copy.wait()

    def arrived(copies):
        for copy in copies:
            copy.wait_recv()

    row_of = [HALF * c + GROUP * a + BLOCK * lax.rem(b + s, 4) for s in (opposite, right, left, 0)]
    grp_copies = []
    for j, row in enumerate(row_of):
        head = pl.multiple_of(row, 16)
        tail = pl.multiple_of(jnp.minimum(row + CUT, SHARD - (BLOCK - CUT)), 16)
        grp_copies.append(local(e_ref.at[pl.ds(head, CUT)], e_grp.at[j, pl.ds(0, CUT)]))
        grp_copies.append(local(e_ref.at[pl.ds(tail, BLOCK - CUT)], e_grp.at[j, pl.ds(CUT, BLOCK - CUT)]))

    def fetch(k):
        rows = pl.ds(pl.multiple_of(start + lax.rem(k, 5) * E_TILE, 32), E_TILE)
        slot = lax.rem(k, 2)
        return pltpu.make_async_copy(e_ref.at[rows], e_tile.at[slot], e_sem.at[slot])

    def chunks(body, size=64):
        def step(i, carry):
            return body(pl.ds(pl.multiple_of(i * size, size), size), carry)
        return lambda carry=0: lax.fori_loop(0, TOK // size, step, carry)

    fetch(0).start()
    start_all(grp_copies)
    barrier = pltpu.get_barrier_semaphore()
    peers = [sib] + [ring[s] for ring in (ring_a, ring_b, ring_x) for s in STEPS]
    for peer in peers:
        pl.semaphore_signal(barrier, inc=1, device_id=peer, device_id_type=MESH_ID)

    gamma, beta = gamma_ref[...], beta_ref[...]

    def x_hat_of(rows):
        value = hid_ref[rows].astype(jnp.float32)
        centered = value - jnp.mean(value, axis=-1, keepdims=True)
        inv = lax.rsqrt(jnp.mean(centered * centered, axis=-1, keepdims=True) + LAYER_EPS)
        return centered * inv, inv

    def norm(rows, carry):
        x_hat, _ = x_hat_of(rows)
        normed = (x_hat * gamma + beta).astype(jnp.bfloat16)
        zb[c, rows] = normed
        zf[rows] = normed.astype(jnp.float32)
        return carry

    chunks(norm)()
    for ref, at in ((st_c, c), (st_x, x), (inf, 0)):
        ref[at] = jnp.zeros((2, 8, TOK), jnp.float32)
    tag[c] = tags_ref[...]
    pl.semaphore_wait(barrier, len(peers))

    tag_copy = remote(tags_ref, tag.at[c], sib)
    own_sib = remote(zf, zf_sib, sib)
    own_right, own_left = (remote(zf, land.at[i], ring_a[s]) for i, s in enumerate((left, right)))
    sib_right, sib_left = (remote(zf_sib, land.at[2 + i], ring_a[s]) for i, s in enumerate((left, right)))
    fwd_own = remote(land.at[1], land.at[4], ring_a[right])
    fwd_sib = remote(land.at[2], land.at[5], ring_a[left])
    start_all([tag_copy, own_sib, own_left, own_right])

    def zero(rows, carry):
        for j in range(4):
            acc[j, rows] = jnp.zeros((80, DIM), jnp.float32)
        return carry

    lax.fori_loop(0, BLOCK // 80, lambda i, carry: zero(pl.ds(pl.multiple_of(i * 80, 80), 80), carry), 0)
    tag_copy.wait()

    counts[0] = jnp.broadcast_to(jnp.sum(tag[0, 0:1] + tag[1, 0:1]), (8, 128))
    round_1 = [remote(counts.at[0], counts.at[1 + i], ring_b[s]) for i, s in enumerate(STEPS)]
    swap = remote(counts.at[4], counts.at[5], sib)
    round_2 = [remote(counts.at[5], counts.at[6 + i], ring_b[s]) for i, s in enumerate(STEPS)]
    start_all(round_1)
    own_sib.wait_recv()
    start_all([sib_left, sib_right])

    def convert(rows, carry):
        zb[1 - c, rows] = zf_sib[rows].astype(jnp.bfloat16)
        return carry

    chunks(convert)()

    def stats_tile(k, carry):
        top, total = carry
        i = lax.rem(k, 5)
        h = jnp.where(k < 5, c, 1 - c)
        slot = lax.rem(k, 2)
        fetch(k + 1).start()
        fetch(k).wait()
        logits = []
        for at in range(0, E_TILE, T1_SUB):
            part = dot_nt(e_tile[slot, at:at + T1_SUB], zb[h])
            if at < OVERLAP:
                rows = lax.broadcasted_iota(jnp.int32, part.shape, 0) + (i * E_TILE + at)
                part = jnp.where(rows >= low, part, -jnp.inf)
            logits.append(part.reshape(T1_SUB // 8, 8, TOK))
        for part in logits:
            new_top = jnp.maximum(top, jnp.max(part, axis=0))
            total = total * jnp.exp(top - new_top) + jnp.sum(jnp.exp(part - new_top[None]), axis=0)
            top = new_top
        return top, total

    def stats_pass(p, carry):
        init = (jnp.full((8, TOK), -jnp.inf, jnp.float32), jnp.zeros((8, TOK), jnp.float32))
        top, total = lax.fori_loop(5 * p, 5 * p + 5, stats_tile, init)
        h = jnp.where(p == 0, c, 1 - c)
        all_top = jnp.max(top, axis=0, keepdims=True)
        st_c[c, h, 0:1] = all_top
        st_c[c, h, 1:2] = jnp.sum(total * jnp.exp(top - all_top), axis=0, keepdims=True)

        @pl.when(p == 0)
        def _():
            wait_all(round_1)
            counts[4] = in_order(counts)
            swap.start()
        return carry

    lax.fori_loop(0, 2, stats_pass, 0)
    swap.wait()
    start_all(round_2)
    chip_copy = remote(st_c.at[c], st_c.at[c], sib)
    chip_copy.start()
    chip_copy.wait()
    for h in range(2):
        st_x[x, h, 0:1], st_x[x, h, 1:2] = merge(top_total(st_c[0, h]), top_total(st_c[1, h]))
    x_copies = to_ring(st_x.at[x], st_x.at[x], ring_x)
    start_all(x_copies)
    wait_all(round_2)
    token_count = jnp.concatenate([in_order(counts.at[pl.ds(5, 4)])[0:1]] * (TOK // 128), axis=1)
    wait_all(x_copies)
    for h in range(2):
        pairs = [top_total(st_x[i, h]) for i in range(4)]
        top, total = merge(merge(pairs[0], pairs[1]), merge(pairs[2], pairs[3]))
        inf[0, h, 0:1] = top + jnp.log(total)
        inf[0, h, 1:2] = tag[h, 0:1] / token_count
        inf[0, h, 2:3] = tag[h, 1:2]
    inf_copies = [remote(inf.at[0], inf.at[1 + i], ring_a[s]) for i, s in enumerate((left, right, opposite))]
    start_all(inf_copies)
    for h in range(2):
        for n in range(3):
            for at in range(0, TOK, 128):
                lanes = slice(at, at + 128)
                cols[h, n, lanes] = jnp.broadcast_to(inf[0, h, n:n + 1, lanes], (128, 128)).T
    dz_acc[...] = jnp.zeros_like(dz_acc)
    hits[...] = jnp.zeros_like(hits)

    def dz_step(s, carry):
        tile, h = s // 2, lax.rem(s, 2)
        k = 10 + tile
        slot = lax.rem(k, 2)

        @pl.when(h == 0)
        def _():
            fetch(k).wait()

            @pl.when(tile < 4)
            def _():
                fetch(k + 1).start()

        spans = ((0, 768), (768, E_TILE - 768))
        logits = [dot_nt(zb[h], e_tile[slot, at:at + size]) for at, size in spans]
        found = jnp.zeros((8, 128), jnp.float32)
        for (at, size), part in zip(spans, logits):
            for n in range(0, size, 128):
                value = part[:, n:n + 128]
                row = lax.broadcasted_iota(jnp.int32, value.shape, 1) + (tile * E_TILE + at + n)
                probs = jnp.exp(value - cols[h, 0])
                target = row + (start + base) == cols[h, 2].astype(jnp.int32)
                grad = jnp.where(target, probs - 1.0, probs) * cols[h, 1]
                hit = jnp.where(target, value * cols[h, 1], 0.0)
                if at + n < OVERLAP:
                    grad, hit = (jnp.where(row >= low, v, 0.0) for v in (grad, hit))
                g_buf[:, at + n:at + n + 128] = grad.astype(jnp.bfloat16)
                found = found + jnp.sum(hit.reshape(TOK // 8, 8, 128), axis=0)
            dz_acc[h] += jnp.dot(g_buf[:, at:at + size], e_tile[slot, at:at + size], preferred_element_type=jnp.float32)
        hits[...] += found
        return carry

    wait_all(grp_copies)
    lo, hi = pl.ds(0, HALF_BLOCK), pl.ds(HALF_BLOCK, HALF_BLOCK)
    opp_lo, opp_hi = remote(acc.at[0, lo], rs_in.at[0], ring_b[right]), remote(acc.at[0, hi], rs_in.at[1], ring_b[left])
    plain_hi, plain_lo = remote(acc.at[1, hi], rs_in.at[2], ring_b[right]), remote(acc.at[2, lo], rs_in.at[3], ring_b[left])
    sum_lo, sum_hi = remote(rs_out.at[0], rs_in.at[4], ring_b[right]), remote(rs_out.at[1], rs_in.at[5], ring_b[left])

    def stage_copy(piece, part):
        rows = pl.ds(part * (TOK // 2), TOK // 2)
        return pltpu.make_async_copy(land.at[piece, rows], stage.at[part], stage_sem.at[part])

    def grad_piece(q, carry):
        @pl.when(q == 2)
        def _():
            own_left.wait_recv()
            fwd_own.start()

        first = jnp.where(q == 2, 0, t2_early)
        last = jnp.where(q == 6, t2_late, t2_early)
        lax.fori_loop(first, last, dz_step, 0)

        @pl.when(q == 2)
        def _():
            arrived([own_right, sib_right])
            fwd_sib.start()
            wait_all(inf_copies)

        @pl.when(q == 4)
        def _():
            sib_left.wait_recv()

        @pl.when(q == 6)
        def _():
            arrived([fwd_own, fwd_sib])

        odd = lax.rem(q, 2)

        @pl.when((q >= 2) & (odd == 0))
        def _():
            for part in range(2):
                stage_copy(q - 2, part).start()

        @pl.when(q >= 2)
        def _():
            for part in range(2):
                stage_copy(q - 2, part).wait()

                def narrow(i, carry):
                    zb[2 + odd, pl.ds(pl.multiple_of(part * (TOK // 2) + i * 64, 64), 64)] = (
                        stage[part, pl.ds(pl.multiple_of(i * 64, 64), 64)].astype(jnp.bfloat16))
                    return carry

                lax.fori_loop(0, TOK // 128, narrow, 0)

                @pl.when(odd == 0)
                def _():
                    stage_copy(q - 1, part).start()

        other = jnp.where((q == 1) | (q == 4) | (q == 5) | (q == 7), 1, 0)
        h = c * (1 - other) + (1 - c) * other
        zi = jnp.where(q < 2, h, 2 + odd)
        src = jnp.where(q < 2, 0, jnp.where(q < 6, 1 + odd, 3))
        lse = inf[src, h, 0:1]
        scale = inf[src, h, 1:2]
        labels = inf[src, h, 2:3].astype(jnp.int32)

        def pair(jj, carry):
            @pl.when((q == 7) & (jj == 1))
            def _():
                start_all([opp_lo, opp_hi, plain_hi])

            logits = [dot_nt(e_grp[2 * jj + i], zb[zi]) for i in range(2)]
            for i in range(2):
                row = jnp.where(jj == 0, row_of[i], row_of[2 + i])
                ids = lax.broadcasted_iota(jnp.int32, (BLOCK, TOK), 0) + (row + base)
                probs = jnp.exp(logits[i] - lse)
                grad = (jnp.where(ids == labels, probs - 1.0, probs) * scale).astype(jnp.bfloat16)
                acc[2 * jj + i] += jnp.dot(grad, zb[zi], preferred_element_type=jnp.float32)
            return carry

        lax.fori_loop(0, 2, pair, 0)
        return carry

    lax.fori_loop(0, 8, grad_piece, 0)

    plain_lo.start()
    opp_lo.wait_recv()
    rs_out[0] = acc[1, lo] + rs_in[0]
    sum_lo.start()
    opp_hi.wait_recv()
    rs_out[1] = acc[2, hi] + rs_in[1]
    sum_hi.start()
    lax.fori_loop(t2_late, 10, dz_step, 0)
    dz_copy = remote(dz_acc.at[1 - c], dz_in, sib)
    dz_copy.start()
    arrived([plain_hi, plain_lo, sum_lo, sum_hi])
    block = acc.at[3]
    block[lo] += rs_in[4] + rs_in[3]
    block[hi] += rs_in[2] + rs_in[5]

    mine, lefts, rights = groups
    ring_lo = [remote(block.at[lo], mine[LEFT].at[lo], ring_b[right]), remote(block.at[lo], mine[RIGHT].at[lo], ring_b[left])]
    ring_hi = [remote(block.at[hi], mine[LEFT].at[hi], ring_b[right]), remote(block.at[hi], mine[RIGHT].at[hi], ring_b[left])]
    far_lo = remote(mine[LEFT].at[lo], mine[OPPOSITE].at[lo], ring_b[right])
    far_hi = remote(mine[RIGHT].at[hi], mine[OPPOSITE].at[hi], ring_b[left])
    keep = local(block, mine[OWN])
    spread = [[remote(mine[k] if k else block, lefts[k], ring_a[right]), remote(mine[k] if k else block, rights[k], ring_a[left])]
              for k in range(4)]
    across = [[remote(group[k] if n or k else block, other[k], sib) for k in range(4)] for n, (group, other) in enumerate(zip(groups, others))]
    start_all(ring_lo + ring_hi + spread[OWN] + [keep, across[0][OWN]])

    dz_copy.wait_recv()
    for copy in (own_sib, own_left, own_right):
        copy.wait_send()

    def add_half(rows, carry):
        dz_in[rows] += dz_acc[c, rows]
        return carry

    chunks(add_half)()

    def quarter(i):
        return pl.ds(pl.multiple_of(i * QUARTER, QUARTER), QUARTER)

    parts = [remote(dz_in.at[quarter(lax.rem(x + s, 4))], x_parts.at[x], ring_x[s]) for s in STEPS]
    hit_copies = to_ring(hits, x_hits.at[x], ring_x)
    start_all(parts + hit_copies)
    x_parts[x] = dz_in[quarter(x)]
    x_hits[x] = hits[...]

    arrived(ring_lo + ring_hi)
    start_all([far_lo, far_hi] + spread[LEFT] + spread[RIGHT] + [across[0][LEFT], across[0][RIGHT]])

    wait_all(parts + hit_copies)
    zf[quarter(x)] = in_order(x_parts)
    wholes = to_ring(zf.at[quarter(x)], zf.at[quarter(x)], ring_x)
    start_all(wholes)
    arrived([far_lo, far_hi])
    start_all(spread[OPPOSITE] + [across[0][OPPOSITE]])
    wait_all(wholes)

    def norm_back(rows, carry):
        d_gamma, d_beta = carry
        x_hat, inv = x_hat_of(rows)
        dz = zf[rows]
        grad = dz * gamma
        grad = grad - jnp.mean(grad, axis=-1, keepdims=True) - x_hat * jnp.mean(grad * x_hat, axis=-1, keepdims=True)
        dh_out[rows] = (grad * inv).astype(jnp.bfloat16)
        rows8 = lambda v: jnp.sum(v.reshape(8, 8, DIM), axis=0)
        return d_gamma + rows8(dz * x_hat), d_beta + rows8(dz)

    zeros = jnp.zeros((8, DIM), jnp.float32)
    d_gamma, d_beta = chunks(norm_back)((zeros, zeros))
    loss = jnp.sum(inf[0, c, 0:1] * inf[0, c, 1:2]) - jnp.sum(in_order(x_hits))
    t_core[c] = zeros
    t_core[c, 0:1] = jnp.sum(d_gamma, axis=0, keepdims=True)
    t_core[c, 1:2] = jnp.sum(d_beta, axis=0, keepdims=True)
    t_core[c, 2:3] = jnp.broadcast_to(loss, (1, DIM))

    between = remote(t_core.at[c], t_core.at[c], sib)
    between.start()
    arrived([spread[OWN][0], spread[OWN][1]])
    start_all([across[1][OWN], across[2][OWN]])
    between.wait()
    t_ring[0, b] = t_core[0] + t_core[1]
    ring_1 = to_ring(t_ring.at[0, b], t_ring.at[0, b], ring_b)
    start_all(ring_1)
    wait_all(ring_1)
    t_swap[0] = in_order(t_ring.at[0])
    crossing = remote(t_swap.at[0], t_swap.at[1], sib)
    crossing.start()
    crossing.wait()
    t_ring[1, b] = t_swap[1]
    ring_2 = to_ring(t_ring.at[1, b], t_ring.at[1, b], ring_b)
    start_all(ring_2)
    wait_all(ring_2)
    t_swap[2 + c] = in_order(t_ring.at[1])
    settle = remote(t_swap.at[2 + c], t_swap.at[2 + c], sib)
    settle.start()
    settle.wait()
    tail_out[...] = t_swap[2]

    for k in (RIGHT, LEFT, OPPOSITE):
        arrived(spread[k])
        start_all([across[1][k], across[2][k]])
    keep.wait()
    for copies in across:
        arrived(copies)
    for copies in across + spread + [ring_lo, ring_hi, [far_lo, far_hi, sib_left, sib_right, fwd_own, fwd_sib, dz_copy,
                                                        opp_lo, opp_hi, plain_lo, plain_hi, sum_lo, sum_hi]]:
        for copy in copies:
            copy.wait_send()


def head(hidden, ln_gamma, ln_beta, tags, embed):
    f32, bf16 = jnp.float32, jnp.bfloat16
    vmem = pl.BlockSpec(memory_space=pltpu.VMEM)
    hbm = pl.BlockSpec(memory_space=pl.ANY)
    blocks = 24
    scratch = [
        ((TOK, DIM), f32),
        ((TOK, DIM), f32),
        ((2, TOK // 2, DIM), f32),
        ((4, TOK, DIM), bf16),
        ((4, BLOCK, DIM), bf16),
        ((2, E_TILE, DIM), bf16),
        ((4, BLOCK, DIM), f32),
        ((2, TOK, DIM), f32),
        ((TOK, DIM), f32),
        ((4, QUARTER, DIM), f32),
        ((TOK, E_TILE), bf16),
        ((2, 3, TOK, 128), f32),
        ((2, 8, TOK), f32),
        ((4, 2, 8, TOK), f32),
        ((2, 2, 8, TOK), f32),
        ((4, 2, 8, TOK), f32),
        ((9, 8, 128), f32),
        ((6, HALF_BLOCK, DIM), f32),
        ((2, HALF_BLOCK, DIM), f32),
        ((8, 128), f32),
        ((4, 8, 128), f32),
        ((2, 8, DIM), f32),
        ((2, 4, 8, DIM), f32),
        ((4, 8, DIM), f32),
    ]
    outs = [((TOK, DIM), bf16), ((8, DIM), f32), ((6, TOK, DIM), f32)] + [((BLOCK, DIM), f32)] * blocks
    return pl.pallas_call(
        functools.partial(head_kernel, t2_early=T2_EARLY, t2_late=T2_LATE),
        name='head',
        out_shape=[jax.ShapeDtypeStruct(*s) for s in outs],
        in_specs=[vmem] * 4 + [hbm],
        out_specs=[vmem] * 2 + [hbm] * (1 + blocks),
        scratch_shapes=[pltpu.VMEM(*s) for s in scratch] + [pltpu.SemaphoreType.DMA((n,)) for n in (2, 2, SEMS)],
        compiler_params=pltpu.CompilerParams(vmem_limit_bytes=KERNEL_VMEM, collective_id=0, has_side_effects=True),
        cost_estimate=pl.CostEstimate(flops=100_000_000_000, bytes_accessed=200_000_000, transcendentals=0),
    )(hidden, ln_gamma[None], ln_beta[None], tags, embed)


def place_kernel(*refs, count):
    at_ref, srcs, out_ref = refs[0], refs[1:1 + count], refs[-4]
    buf, in_sems, out_sems = refs[-3:]
    parts = (pl.ds(0, CUT), pl.ds(CUT, BLOCK - CUT))

    def read(j, k):
        return pltpu.make_async_copy(srcs[j].at[parts[k]], buf.at[j, parts[k]], in_sems.at[j, k])

    def write(j, k):
        rows = pl.ds(pl.multiple_of(at_ref[2 * j] + k * CUT, 16), parts[k].size)
        return pltpu.make_async_copy(buf.at[j, parts[k]], out_ref.at[rows], out_sems.at[j, k])

    def each(action):
        for j in range(count):
            for k in range(2):
                action(j, k)

    def forward(j, k):
        read(j, k).wait()
        pl.when((at_ref[2 * j + 1] == 1) | (k == 0))(lambda: write(j, k).start())

    each(lambda j, k: read(j, k).start())
    each(forward)
    each(lambda j, k: pl.when((at_ref[2 * j + 1] == 1) | (k == 0))(lambda: write(j, k).wait()))


def place(at, blocks, out):
    count = len(blocks)
    any_spec = pl.BlockSpec(memory_space=pl.ANY)
    old = [] if out is None else [out]
    return pl.pallas_call(
        functools.partial(place_kernel, count=count),
        name=f'place_{count}',
        out_shape=jax.ShapeDtypeStruct((SHARD, DIM), jnp.float32),
        in_specs=[pl.BlockSpec(memory_space=pltpu.SMEM)] + [any_spec] * (count + len(old)),
        out_specs=any_spec,
        input_output_aliases={1 + count: 0} if old else {},
        scratch_shapes=[
            pltpu.VMEM((count, BLOCK, DIM), jnp.float32),
            pltpu.SemaphoreType.DMA((count, 2)),
            pltpu.SemaphoreType.DMA((count, 2)),
        ],
        compiler_params=pltpu.CompilerParams(vmem_limit_bytes=VMEM_LIMIT),
        cost_estimate=pl.CostEstimate(flops=count * PLACE_FLOPS, bytes_accessed=count * BLOCK * DIM * 8, transcendentals=0),
    )(at, *blocks, *old)


def block_rows(c, a, b):
    a, b = a % 4, b % 4
    row = HALF * c + GROUP * a + BLOCK * b
    full = 1 - ((c == 1) & (a == 3) & (b == 3)).astype(jnp.int32)
    return row, full


def place_at(c, a, b, steps):
    values = []
    for s in steps:
        values.extend(block_rows(c, a, b + s))
    return jnp.stack(values).astype(jnp.int32)


def solution(mesh):
    mesh4 = Mesh(mesh.devices.reshape(SIZES), AXES)

    def local_step(hidden, ln_gamma, ln_beta, embed, labels, loss_mask):
        rows = jnp.concatenate([loss_mask, labels], axis=0).astype(jnp.float32)
        tags = jnp.concatenate([rows, jnp.zeros((6, TOK), jnp.float32)], axis=0)
        d_hidden, tail, _, *blocks = head(hidden[0], ln_gamma, ln_beta, tags, embed)
        mine, lefts, rights, sib_mine, sib_lefts, sib_rights = (blocks[i:i + 4] for i in range(0, 24, 4))
        x, z, y, c = (lax.axis_index(n) for n in AXES)
        a = jnp.where(c == 0, y, z)
        b = jnp.where(c == 0, z, y)

        far = [send(lefts[OWN], RING_RIGHT), send(rights[OPPOSITE], RING_LEFT),
               send(lefts[RIGHT], RING_RIGHT), send(rights[LEFT], RING_LEFT)]
        order = (OWN, OPPOSITE, RIGHT, LEFT)
        everything = range(4)

        def place_pair(a_step, steps, own_blocks, sib_blocks, out):
            at = jnp.concatenate([place_at(c, a + a_step, b, steps), place_at(1 - c, b + a_step, a, steps)])
            return place(at, own_blocks + sib_blocks, out)

        out = place_pair(0, everything, mine, sib_mine, None)
        out = place_pair(-1, everything, lefts, sib_lefts, out)
        far_1, out = lax.optimization_barrier((far[:2], out))
        sib_1 = [send(block, SIB) for block in far_1]
        out = place_pair(1, everything, rights, sib_rights, out)
        far_2, out = lax.optimization_barrier((far[2:], out))
        sib_2 = [send(block, SIB) for block in far_2]
        out = place_pair(2, order[:2], far_1, sib_1, out)
        out = place_pair(2, order[2:], far_2, sib_2, out)
        return tail[2, 0], d_hidden[None], out, tail[0], tail[1]

    dp = ('z', 'y', 'c')
    return jax.shard_map(
        local_step, mesh=mesh4,
        in_specs=(P(dp, None, None), P(None), P(None), P('tp', None), P(dp, None), P(dp, None)),
        out_specs=(P(), P(dp, None, None), P('tp', None), P(None), P(None)),
        check_vma=False)
```
